512 devices in a mesh: rep: 2 (over y), tp: 32 (over z), ep: 8 (over x, core).
Axes of the slice: x: 4, y: 2, z: 32, core: 2. Of those that a mesh axis runs over, the one named last changes fastest.
The devices are a block of a 4x8x32 slice.
Arguments:
- tokens: bfloat16 [1536, 3072], P(('rep', 'ep'), 'tp'), parts along dimension 0, may hold values from -6 to 6
- routing: int32 [1536, 2], P(('rep', 'ep')), parts along dimension 0, may hold values from 0 to 7, all different within a row; in each aligned block of 96 rows (0 to 95, 96 to 191, ...) at most 30 rows name the same one
- route_gates: float32 [1536, 2], P(('rep', 'ep')), parts along dimension 0, may hold values from 0.2 to 1
- expert_gate: bfloat16 [8, 3072, 8192], P('ep', None, 'tp'), may hold values from -0.109375 to 0.109375
- expert_up: bfloat16 [8, 3072, 8192], P('ep', None, 'tp'), may hold values from -0.109375 to 0.109375
- expert_down: bfloat16 [8, 8192, 3072], P('ep', 'tp'), may hold values from -0.0625 to 0.0625
Outputs:
- mixture: bfloat16 [1536, 3072], P(('rep', 'ep'), 'tp'), parts along dimension 0
The draws below stay inside these ranges and needn't reach their ends.
There are 2 independent parts, one for each index of `rep`. The reference program is written for one: setup_inputs(seed, part) draws one part's arguments, and reference() takes and returns one part's arrays. A program takes and returns all parts, laid end to end along the dimension named above; an argument that names none is the same for every part. Nothing has to cross between parts.
Inputs may be any that keep to these rules, and one draw needn't show every extreme that they name: `routing`: each token names two different experts. In each aligned block of 96 tokens (the rows of one index of ep) no expert is named by more than 30 tokens, a bound that some block reaches.
All inputs are finite; a program needn't handle non-finite values.
Results may differ from the reference program's by a relative error of at most 0.0085.
Values may be sent and summed in bfloat16 or wider, within the bound.
No kernel may reach another device: no remote copies, remote signals or barrier semaphores. Data moves between devices by JAX's collectives and lax.ppermute only.
A program may use at most 64 MiB of HBM per device.

```python
import math
import jax
import jax.numpy as jnp
import numpy as np
from jax import lax

D = 3072
FF = 8192
TOK_DEV = 96
EXPERTS = 8
CAP = 30
TOKENS = 768


def shard_levels(key, extent, split, least, top_value):
    factor_of, own = 1.0, jax.random.fold_in(key, 6)
    for dim, blocks in split:
        draws = jnp.exp(jax.random.uniform(jax.random.fold_in(own, dim), (blocks,), jnp.float32, least / len(split), top_value / len(split)))
        factor_of = factor_of * jnp.repeat(draws, extent[dim] // blocks).reshape([-1 if axis == dim else 1 for axis in range(len(extent))])
    return factor_of


def routed_block(rng, own, number, rows, number_of, top, limit, slope):
    order = jax.random.permutation(rng, number_of)
    heavy_load, ordinary = load_shares(number_of, rows * top, limit, slope, True), load_shares(number_of, rows * top, limit, slope, False)
    places = jnp.arange(number_of)

    def named(sizes, offset_by):
        used = int((sizes > 0).sum())
        fixed = max(1, used // 4)
        moved = fixed + (places - fixed + offset_by * (used - fixed)) % max(1, number_of - fixed)
        return jnp.zeros((number_of,), jnp.int32).at[order[jnp.where(places < fixed, places, moved)]].set(jnp.asarray(sizes, jnp.int32))

    sizes = jnp.where(number % 4 == 0, named(heavy_load, number // 4), named(ordinary, number - number // 4 - 1))
    mixed = jax.random.permutation(jax.random.fold_in(own, 3), number_of)
    giver, sink = mixed[0:number_of // 2 * 2:2], mixed[1:number_of // 2 * 2:2]
    room = jnp.minimum(sizes[giver] - 1, limit - sizes[sink]) // 2
    room = jnp.where((giver == order[0]) | (sink == order[0]) | (sizes[sink] == 0), 0, jnp.maximum(room, 0))
    moved = jax.random.randint(jax.random.fold_in(own, 4), (number_of // 2,), 0, 1 << 20) % (room + 1)
    sizes = sizes.at[giver].add(-moved).at[sink].add(moved)
    members = jnp.searchsorted(jnp.cumsum(sizes), jnp.arange(rows * top), side="right").astype(jnp.int32)
    grid = members.reshape(top, rows).T
    grid = grid[jax.random.permutation(jax.random.fold_in(own, 1), rows)]
    offset_by = jax.random.randint(jax.random.fold_in(own, 2), (rows, 1), 0, top)
    return jnp.take_along_axis(grid, (jnp.arange(top)[None, :] + offset_by) % top, axis=1)


def load_shares(number_of, total, most, slope, full):
    portions = [(1 << 20) // math.isqrt(rank ** slope) + 1 for rank in range(1, number_of + 1)]
    largest = most if full else min(most, max(-(-total // number_of), total * portions[0] // sum(portions)))
    least = 1 if total - largest >= number_of - 1 else 0
    holding, spare = [largest] + [least] * (number_of - 1), total - largest - least * (number_of - 1)
    while spare > 0:
        movable = [i for i in range(1, number_of) if holding[i] < largest] or [i for i in range(1, number_of) if holding[i] < most]
        mass, remaining = sum([portions[i] for i in movable]), spare
        for i in movable:
            addition = min(most - holding[i], max(1, remaining * portions[i] // mass), spare)
            holding[i] = holding[i] + addition
            spare = spare - addition
    return np.array(holding)


def gaussian(stream_key, extent, scale, most, cuts=(), held_as=jnp.bfloat16):
    result = jax.random.normal(stream_key, extent, jnp.float32) * scale
    if len(cuts) > 0:
        result = shard_levels(stream_key, extent, cuts, -0.22, 0.18) * result
    return jnp.clip(result, min=-most, max=most).astype(held_as)


def setup_inputs(seed: int = 0, part: int = 0) -> dict:
    seeds = jax.random.split(jax.random.key(seed), 7)
    part_splits = jax.random.split(jax.random.fold_in(seeds[6], part), 7)
    tokens = gaussian(part_splits[0], (TOKENS, D), 1.0, 6.0, ((0, 8), (1, 32)))
    routing_keys = jax.random.split(jax.random.fold_in(part_splits[1], 1), TOKENS // TOK_DEV)
    routing_turns = jax.random.permutation(jax.random.fold_in(part_splits[1], 3), TOKENS // TOK_DEV)
    routing = jax.vmap(lambda own, number: routed_block(jax.random.fold_in(part_splits[1], 2), own, number, TOK_DEV, EXPERTS, 2, CAP, 2))(routing_keys, routing_turns).reshape((TOKENS, 2))
    route_gates = jnp.clip(0.2 + 0.8 * jax.random.uniform(part_splits[2], (TOKENS, 2), jnp.float32) ** shard_levels(part_splits[2], (TOKENS, 2), ((0, 8),), -0.2, 0.2), 0.2, 1.0)
    expert_gate = gaussian(seeds[3], (EXPERTS, D, FF), D ** -0.5, 0.109375, ((0, 8), (2, 32)))
    expert_up = gaussian(seeds[4], (EXPERTS, D, FF), D ** -0.5, 0.109375, ((0, 8), (2, 32)))
    expert_down = gaussian(seeds[5], (EXPERTS, FF, D), FF ** -0.5, 0.0625, ((0, 8), (1, 32)))
    return {"tokens": tokens, "routing": routing, "route_gates": route_gates, "expert_gate": expert_gate, "expert_up": expert_up, "expert_down": expert_down}


def slot_tables(routing, route_gates):
    count_rows = routing.shape[0]
    choices_n = routing.shape[1]
    flat_ids = routing.reshape(-1).astype(jnp.int32)
    onehot = (flat_ids[:, None] == jnp.arange(EXPERTS, dtype=jnp.int32)[None, :]).astype(jnp.int32)
    before = jnp.cumsum(onehot, axis=0) - onehot
    position = jnp.sum(before * onehot, axis=1)
    slot_index = flat_ids * CAP + position
    picked = (slot_index[:, None] == jnp.arange(EXPERTS * CAP, dtype=jnp.int32)[None, :]).astype(jnp.float32)
    dispatch = picked.reshape(count_rows, choices_n, EXPERTS * CAP).sum(axis=1)
    combine = (picked * route_gates.reshape(-1)[:, None]).reshape(count_rows, choices_n, EXPERTS * CAP).sum(axis=1)
    return dispatch, combine


def one_expert(operands):
    row_block, w_gate, w_upward, w_down = operands
    gate_part = jnp.dot(row_block, w_gate, preferred_element_type=jnp.float32)
    upward = jnp.dot(row_block, w_upward, preferred_element_type=jnp.float32)
    hidden = (jax.nn.silu(gate_part) * upward).astype(jnp.bfloat16)
    return jnp.dot(hidden, w_down, preferred_element_type=jnp.float32).astype(jnp.bfloat16)


def reference(tokens, routing, route_gates, expert_gate, expert_up, expert_down):
    blocks = TOKENS // TOK_DEV
    dispatch, combine = jax.vmap(slot_tables)(routing.reshape(blocks, TOK_DEV, 2), route_gates.reshape(blocks, TOK_DEV, 2))
    block_tokens = tokens.reshape(blocks, TOK_DEV, D).astype(jnp.float32)
    packed = jnp.einsum('btc,btd->bcd', dispatch, block_tokens, precision=lax.Precision.HIGHEST).astype(jnp.bfloat16)
    expert_rows = packed.reshape(blocks, EXPERTS, CAP, D).transpose(1, 0, 2, 3).reshape(EXPERTS, blocks * CAP, D)
    expert_out = lax.map(one_expert, (expert_rows, expert_gate, expert_up, expert_down))
    back = expert_out.reshape(EXPERTS, blocks, CAP, D).transpose(1, 0, 2, 3).reshape(blocks, EXPERTS * CAP, D)
    mixed = jnp.einsum('btc,bcd->btd', combine, back.astype(jnp.float32), precision=lax.Precision.HIGHEST)
    return mixed.reshape(TOKENS, D).astype(jnp.bfloat16)
```

```python
import jax
import jax.numpy as jnp
from jax import lax
from jax.sharding import Mesh
from jax.sharding import PartitionSpec as P

REP_EP = ("rep", "ep")
TP = ("hi", "lo")
BF = jnp.bfloat16
F32 = jnp.float32
LO = 2


def slot_tables(routing, route_gates, experts, rows):
    tok_count, choices_n = routing.shape
    flat_ids = routing.reshape(-1)
    onehot = (flat_ids[:, None] == jnp.arange(experts, dtype=jnp.int32)[None, :]).astype(BF)
    n = tok_count * choices_n
    earlier = (jnp.arange(n)[None, :] < jnp.arange(n)[:, None]).astype(BF)
    before = jnp.dot(earlier, onehot, preferred_element_type=F32)
    position = jnp.sum(before * onehot.astype(F32), axis=1).astype(jnp.int32)
    slot = (flat_ids * rows + position).reshape(tok_count, choices_n)
    picked = slot[:, :, None] == jnp.arange(experts * rows, dtype=jnp.int32)[None, None, :]
    dispatch = picked.astype(F32).sum(axis=1).astype(BF)
    combine = jnp.where(picked, route_gates[:, :, None], 0.0).sum(axis=1)
    return dispatch, combine


def body(tokens, routing, route_gates, expert_gate, expert_up, expert_down):
    ep_count = lax.axis_size("ep")
    hi_count = lax.axis_size("hi")
    tok_count, feat = tokens.shape
    capacity = 2 * tok_count // ep_count + tok_count // 16
    rows = -(-capacity // 8) * 8
    slots = ep_count * rows
    wide = hi_count * feat
    hidden_n = expert_gate.shape[2]

    own = jnp.broadcast_to(tokens.T[None], (hi_count, feat, tok_count))
    gathered = lax.all_to_all(own, "hi", 0, 0, tiled=True).reshape(wide, tok_count)
    dispatch, combine = slot_tables(routing, route_gates, ep_count, rows)
    packed = lax.dot_general(
        dispatch, gathered, (((0,), (1,)), ((), ())), preferred_element_type=F32
    ).astype(BF)
    sent = jnp.broadcast_to(packed.reshape(1, ep_count, rows, wide), (LO, ep_count, rows, wide))
    got = lax.all_to_all(
        sent.reshape(LO * ep_count, rows, wide), ("lo", "ep"), 0, 0, tiled=True
    ).reshape(LO, slots, wide)

    def by_lo(w):
        return w.reshape(hi_count, LO, feat, hidden_n).transpose(1, 0, 2, 3).reshape(LO, wide, hidden_n)

    w_gate, w_up = by_lo(expert_gate), by_lo(expert_up)
    gate = sum(jnp.dot(got[i], w_gate[i], preferred_element_type=F32) for i in range(LO))
    up = sum(jnp.dot(got[i], w_up[i], preferred_element_type=F32) for i in range(LO))
    hidden = (jax.nn.silu(gate) * up).astype(BF)

    w_down = (
        expert_down.reshape(hidden_n, hi_count, LO, feat)
        .transpose(2, 0, 1, 3)
        .reshape(LO, hidden_n, wide)
    )
    part = jnp.stack([jnp.dot(hidden, w_down[i], preferred_element_type=F32).astype(BF) for i in range(LO)])
    back = lax.all_to_all(
        part.reshape(LO * ep_count, rows, wide), ("lo", "ep"), 0, 0, tiled=True
    ).reshape(LO * slots, wide)
    weights = jnp.concatenate([combine] * LO, axis=1).astype(BF)
    mixed = lax.dot_general(
        back, weights, (((0,), (1,)), ((), ())), preferred_element_type=F32
    ).astype(BF)
    shares = lax.all_to_all(
        mixed.reshape(hi_count, feat, tok_count), "hi", 0, 0, tiled=True
    )
    return jnp.sum(shares.astype(F32), axis=0).astype(BF).T


def solution(mesh):
    finer = Mesh(
        mesh.devices.reshape(
            mesh.shape["rep"], mesh.shape["tp"] // LO, LO, mesh.shape["ep"]
        ),
        ("rep", "hi", "lo", "ep"),
    )
    placed = (
        P(REP_EP, TP),
        P(REP_EP, None),
        P(REP_EP, None),
        P("ep", None, TP),
        P("ep", None, TP),
        P("ep", TP, None),
    )
    return jax.shard_map(
        body, mesh=finer, in_specs=placed, out_specs=P(REP_EP, TP), check_vma=False
    )
```

```python
import jax
import jax.numpy as jnp
from jax import lax
from jax.sharding import Mesh
from jax.sharding import PartitionSpec as P

REP_EP = ("rep", "ep")
TP = ("hi", "lo")
BF = jnp.bfloat16
F32 = jnp.float32
LO = 2


def slot_tables(routing, route_gates, experts, rows):
    tok_count, choices_n = routing.shape
    flat_ids = routing.reshape(-1)
    onehot = (flat_ids[:, None] == jnp.arange(experts, dtype=jnp.int32)[None, :]).astype(BF)
    n = tok_count * choices_n
    earlier = (jnp.arange(n)[None, :] < jnp.arange(n)[:, None]).astype(BF)
    before = jnp.dot(earlier, onehot, preferred_element_type=F32)
    position = jnp.sum(before * onehot.astype(F32), axis=1).astype(jnp.int32)
    slot = (flat_ids * rows + position).reshape(tok_count, choices_n)
    picked = slot[:, :, None] == jnp.arange(experts * rows, dtype=jnp.int32)[None, None, :]
    dispatch = picked.astype(F32).sum(axis=1).astype(BF)
    combine = jnp.where(picked, route_gates[:, :, None], 0.0).sum(axis=1)
    return dispatch, combine


def body(tokens, routing, route_gates, expert_gate, expert_up, expert_down):
    ep_count = lax.axis_size("ep")
    hi_count = lax.axis_size("hi")
    tok_count, feat = tokens.shape
    capacity = 2 * tok_count // ep_count + tok_count // 16
    rows = -(-capacity // 8) * 8
    slots = ep_count * rows
    wide = hi_count * feat
    hidden_n = expert_gate.shape[2]

    gathered = lax.all_gather(tokens.T, "hi", axis=0, tiled=True)
    dispatch, combine = slot_tables(routing, route_gates, ep_count, rows)
    packed = lax.dot_general(
        dispatch, gathered, (((0,), (1,)), ((), ())), preferred_element_type=F32
    ).astype(BF)
    sent = jnp.broadcast_to(packed.reshape(1, ep_count, rows, wide), (LO, ep_count, rows, wide))
    got = lax.all_to_all(
        sent.reshape(LO * ep_count, rows, wide), ("lo", "ep"), 0, 0, tiled=True
    ).reshape(LO, slots, wide)

    def by_lo(w):
        return w.reshape(hi_count, LO, feat, hidden_n).transpose(1, 0, 2, 3).reshape(LO, wide, hidden_n)

    w_gate, w_up = by_lo(expert_gate), by_lo(expert_up)
    gate = sum(jnp.dot(got[i], w_gate[i], preferred_element_type=F32) for i in range(LO))
    up = sum(jnp.dot(got[i], w_up[i], preferred_element_type=F32) for i in range(LO))
    hidden = (jax.nn.silu(gate) * up).astype(BF)

    w_down = (
        expert_down.reshape(hidden_n, hi_count, LO, feat)
        .transpose(2, 0, 1, 3)
        .reshape(LO, hidden_n, wide)
    )
    part = jnp.stack([jnp.dot(hidden, w_down[i], preferred_element_type=F32).astype(BF) for i in range(LO)])
    back = lax.all_to_all(
        part.reshape(LO * ep_count, rows, wide), ("lo", "ep"), 0, 0, tiled=True
    ).reshape(LO * slots, wide)
    weights = jnp.concatenate([combine] * LO, axis=1).astype(BF)
    mixed = lax.dot_general(
        back, weights, (((0,), (1,)), ((), ())), preferred_element_type=F32
    ).astype(BF)
    shares = lax.all_to_all(
        mixed.reshape(hi_count, feat, tok_count), "hi", 0, 0, tiled=True
    )
    return jnp.sum(shares.astype(F32), axis=0).astype(BF).T


def solution(mesh):
    finer = Mesh(
        mesh.devices.reshape(
            mesh.shape["rep"], mesh.shape["tp"] // LO, LO, mesh.shape["ep"]
        ),
        ("rep", "hi", "lo", "ep"),
    )
    placed = (
        P(REP_EP, TP),
        P(REP_EP, None),
        P(REP_EP, None),
        P("ep", None, TP),
        P("ep", None, TP),
        P("ep", TP, None),
    )
    return jax.shard_map(
        body, mesh=finer, in_specs=placed, out_specs=P(REP_EP, TP), check_vma=False
    )
```

```python
import functools

import jax
import jax.numpy as jnp
from jax import lax
from jax.experimental import pallas as pl
from jax.experimental.pallas import tpu as pltpu
from jax.sharding import Mesh
from jax.sharding import PartitionSpec as P

REP_EP = ("rep", "ep")
TP = ("hi", "lo")
BF = jnp.bfloat16
F32 = jnp.float32
LO = 2


def held_close(value):
    return pltpu.with_memory_space_constraint(value, pltpu.VMEM)


def slot_match(routing_ref, experts, rows):
    tok_count = routing_ref.shape[1]
    shape = (experts * rows, tok_count)
    slot = lax.broadcasted_iota(jnp.int32, shape, 0)
    expert, place = slot // rows, slot % rows
    named = (routing_ref[0:1, :] == expert) | (routing_ref[1:2, :] == expert)
    square = (tok_count, tok_count)
    earlier = lax.broadcasted_iota(jnp.int32, square, 0) < lax.broadcasted_iota(jnp.int32, square, 1)
    before = jnp.dot(
        named.astype(F32).astype(BF), earlier.astype(F32).astype(BF), preferred_element_type=F32
    )
    return expert, named & (before == place.astype(F32))


def pack_kernel(experts, rows, routing_ref, tokens_ref, out_ref, whole_ref):
    hi_count, _, feat = tokens_ref.shape
    _, held = slot_match(routing_ref, experts, rows)
    dispatch = held.astype(F32).astype(BF)
    for i in range(hi_count):
        whole_ref[:, i * feat : (i + 1) * feat] = tokens_ref[i]
    packed = jnp.dot(dispatch, whole_ref[...], preferred_element_type=F32).astype(BF)
    for i in range(out_ref.shape[0]):
        out_ref[i] = packed


def combine_kernel(experts, rows, routing_ref, gates_ref, back_ref, out_ref):
    hi_count, _, feat = out_ref.shape
    expert, held = slot_match(routing_ref, experts, rows)
    weight = jnp.where(routing_ref[0:1, :] == expert, gates_ref[0:1, :], gates_ref[1:2, :])
    weight = jnp.where(held, weight, 0.0).astype(BF)
    weight = jnp.concatenate([weight] * LO, axis=0)
    mixed = lax.dot_general(
        weight, back_ref[...], (((0,), (0,)), ((), ())), preferred_element_type=F32
    ).astype(BF)
    for i in range(hi_count):
        out_ref[i] = mixed[:, i * feat : (i + 1) * feat]


def body(tokens, routing, route_gates, expert_gate, expert_up, expert_down):
    ep_count = lax.axis_size("ep")
    hi_count = lax.axis_size("hi")
    tok_count, feat = tokens.shape
    capacity = 2 * tok_count // ep_count + tok_count // 16
    rows = -(-capacity // 16) * 16
    slots = ep_count * rows
    wide = hi_count * feat
    hidden_n = expert_gate.shape[2]
    in_vmem = pl.BlockSpec(memory_space=pltpu.VMEM)

    gathered = lax.all_gather(tokens, "hi", axis=0)
    sent = pl.pallas_call(
        functools.partial(pack_kernel, ep_count, rows),
        out_shape=pltpu.VMEM((LO, slots, wide), BF),
        in_specs=[in_vmem, in_vmem],
        out_specs=in_vmem,
        scratch_shapes=[pltpu.VMEM((tok_count, wide), BF)],
        name="pack",
    )(routing.T, held_close(gathered))
    got = lax.all_to_all(
        sent.reshape(LO * ep_count, rows, wide), ("lo", "ep"), 0, 0, tiled=True
    ).reshape(LO, slots, wide)

    def by_lo(w):
        return w.reshape(hi_count, LO, feat, hidden_n).transpose(1, 0, 2, 3).reshape(LO, wide, hidden_n)

    w_gate, w_up = by_lo(expert_gate), by_lo(expert_up)
    gate = sum(jnp.dot(got[i], w_gate[i], preferred_element_type=F32) for i in range(LO))
    up = sum(jnp.dot(got[i], w_up[i], preferred_element_type=F32) for i in range(LO))
    hidden = (jax.nn.silu(gate) * up).astype(BF)

    w_down = (
        expert_down.reshape(hidden_n, hi_count, LO, feat)
        .transpose(2, 0, 1, 3)
        .reshape(LO, hidden_n, wide)
    )
    part = jnp.stack([jnp.dot(hidden, w_down[i], preferred_element_type=F32).astype(BF) for i in range(LO)])
    back = lax.all_to_all(
        part.reshape(LO * ep_count, rows, wide), ("lo", "ep"), 0, 0, tiled=True
    ).reshape(LO * slots, wide)
    mixed = pl.pallas_call(
        functools.partial(combine_kernel, ep_count, rows),
        out_shape=pltpu.VMEM((hi_count, tok_count, feat), BF),
        in_specs=[in_vmem, in_vmem, in_vmem],
        out_specs=in_vmem,
        name="combine",
    )(routing.T, route_gates.T, held_close(back))
    shares = lax.all_to_all(mixed, "hi", 0, 0, tiled=True)
    return jnp.sum(shares.astype(F32), axis=0).astype(BF)


def solution(mesh):
    finer = Mesh(
        mesh.devices.reshape(
            mesh.shape["rep"], mesh.shape["tp"] // LO, LO, mesh.shape["ep"]
        ),
        ("rep", "hi", "lo", "ep"),
    )
    placed = (
        P(REP_EP, TP),
        P(REP_EP, None),
        P(REP_EP, None),
        P("ep", None, TP),
        P("ep", None, TP),
        P("ep", TP, None),
    )
    return jax.shard_map(
        body, mesh=finer, in_specs=placed, out_specs=P(REP_EP, TP), check_vma=False
    )
```

```python
import functools

import jax
import jax.numpy as jnp
from jax import lax
from jax.experimental import pallas as pl
from jax.experimental.pallas import tpu as pltpu
from jax.sharding import Mesh
from jax.sharding import PartitionSpec as P

REP_EP = ("rep", "ep")
TP = ("hi", "lo")
BF = jnp.bfloat16
F32 = jnp.float32
LO = 2


def held_close(value):
    return pltpu.with_memory_space_constraint(value, pltpu.VMEM)


def slot_match(routing_ref, experts, rows):
    tok_count = routing_ref.shape[1]
    shape = (experts * rows, tok_count)
    slot = lax.broadcasted_iota(jnp.int32, shape, 0)
    expert, place = slot // rows, slot % rows
    named = (routing_ref[0:1, :] == expert) | (routing_ref[1:2, :] == expert)
    square = (tok_count, tok_count)
    earlier = lax.broadcasted_iota(jnp.int32, square, 0) < lax.broadcasted_iota(jnp.int32, square, 1)
    before = jnp.dot(
        named.astype(F32).astype(BF), earlier.astype(F32).astype(BF), preferred_element_type=F32
    )
    return expert, named & (before == place.astype(F32))


def pack_kernel(experts, rows, routing_ref, tokens_ref, out_ref, whole_ref):
    hi_count, _, feat = tokens_ref.shape
    _, held = slot_match(routing_ref, experts, rows)
    dispatch = held.astype(F32).astype(BF)
    for i in range(hi_count):
        whole_ref[:, i * feat : (i + 1) * feat] = tokens_ref[i]
    packed = jnp.dot(dispatch, whole_ref[...], preferred_element_type=F32).astype(BF)
    for i in range(out_ref.shape[0]):
        out_ref[i] = packed


def combine_kernel(experts, rows, feat, routing_ref, gates_ref, back_ref, out_ref):
    tok_count = routing_ref.shape[1]
    hi_count = back_ref.shape[1] // feat
    expert, held = slot_match(routing_ref, experts, rows)
    weight = jnp.where(routing_ref[0:1, :] == expert, gates_ref[0:1, :], gates_ref[1:2, :])
    weight = jnp.where(held, weight, 0.0).astype(BF)
    weight = jnp.concatenate([weight] * LO, axis=0)
    mixed = lax.dot_general(
        weight, back_ref[...], (((0,), (0,)), ((), ())), preferred_element_type=F32
    )
    full = tok_count * 3 // 4
    for i in range(hi_count):
        at = (i,)
        block = mixed[:, i * feat : (i + 1) * feat]
        out_ref[*at, :, :feat] = block[:full].astype(BF)
        tail = [block[full:, j * (feat // 3) : (j + 1) * (feat // 3)] for j in range(3)]
        out_ref[*at, :, feat:] = jnp.concatenate(tail, axis=0).astype(BF)


def body(tokens, routing, route_gates, expert_gate, expert_up, expert_down):
    ep_count = lax.axis_size("ep")
    hi_count = lax.axis_size("hi")
    tok_count, feat = tokens.shape
    capacity = 2 * tok_count // ep_count + tok_count // 16
    rows = -(-capacity // 16) * 16
    slots = ep_count * rows
    wide = hi_count * feat
    hidden_n = expert_gate.shape[2]
    in_vmem = pl.BlockSpec(memory_space=pltpu.VMEM)

    gathered = lax.all_gather(tokens, "hi", axis=0)
    sent = pl.pallas_call(
        functools.partial(pack_kernel, ep_count, rows),
        out_shape=pltpu.VMEM((LO, slots, wide), BF),
        in_specs=[in_vmem, in_vmem],
        out_specs=in_vmem,
        scratch_shapes=[pltpu.VMEM((tok_count, wide), BF)],
        name="pack",
    )(routing.T, held_close(gathered))
    got = lax.all_to_all(
        sent.reshape(LO * ep_count, rows, wide), ("lo", "ep"), 0, 0, tiled=True
    ).reshape(LO, slots, wide)

    def by_lo(w):
        return w.reshape(hi_count, LO, feat, hidden_n).transpose(1, 0, 2, 3).reshape(LO, wide, hidden_n)

    w_gate, w_up = by_lo(expert_gate), by_lo(expert_up)
    gate = sum(jnp.dot(got[i], w_gate[i], preferred_element_type=F32) for i in range(LO))
    up = sum(jnp.dot(got[i], w_up[i], preferred_element_type=F32) for i in range(LO))
    hidden = (jax.nn.silu(gate) * up).astype(BF)

    w_down = (
        expert_down.reshape(hidden_n, hi_count, LO, feat)
        .transpose(2, 0, 1, 3)
        .reshape(LO, hidden_n, wide)
    )
    part = jnp.stack([jnp.dot(hidden, w_down[i], preferred_element_type=F32).astype(BF) for i in range(LO)])
    back = lax.all_to_all(
        part.reshape(LO * ep_count, rows, wide), ("lo", "ep"), 0, 0, tiled=True
    ).reshape(LO * slots, wide)
    mixed = pl.pallas_call(
        functools.partial(combine_kernel, ep_count, rows, feat),
        out_shape=pltpu.VMEM((*(hi_count,), tok_count * 3 // 4, feat * 4 // 3), BF),
        in_specs=[in_vmem, in_vmem, in_vmem],
        out_specs=in_vmem,
        name="combine",
    )(routing.T, route_gates.T, held_close(back))
    shares = lax.all_to_all(mixed, "hi", 0, 0, tiled=True)
    return pl.pallas_call(
        finish_kernel,
        out_shape=jax.ShapeDtypeStruct((tok_count, feat), BF),
        in_specs=[in_vmem],
        out_specs=in_vmem,
        name="finish",
    )(held_close(shares))


def finish_kernel(shares_ref, out_ref):
    tok_count, feat = out_ref.shape
    full, cut = tok_count * 3 // 4, feat // 3
    total = jnp.sum(shares_ref[...].astype(F32), axis=0)
    out_ref[:full] = total[:, :feat].astype(BF)
    step = full // 3
    tail = [total[j * step : (j + 1) * step, feat:] for j in range(3)]
    out_ref[full:] = jnp.concatenate(tail, axis=1).astype(BF)


def solution(mesh):
    finer = Mesh(
        mesh.devices.reshape(
            mesh.shape["rep"], mesh.shape["tp"] // LO, LO, mesh.shape["ep"]
        ),
        ("rep", "hi", "lo", "ep"),
    )
    placed = (
        P(REP_EP, TP),
        P(REP_EP, None),
        P(REP_EP, None),
        P("ep", None, TP),
        P("ep", None, TP),
        P("ep", TP, None),
    )
    return jax.shard_map(
        body, mesh=finer, in_specs=placed, out_specs=P(REP_EP, TP), check_vma=False
    )
```

```python
import functools

import jax
import jax.numpy as jnp
from jax import lax
from jax.experimental import pallas as pl
from jax.experimental.pallas import tpu as pltpu
from jax.sharding import Mesh
from jax.sharding import PartitionSpec as P

REP_EP = ("rep", "ep")
TP = ("hi", "lo")
BF = jnp.bfloat16
F32 = jnp.float32
LO = 2


def held_close(value):
    return pltpu.with_memory_space_constraint(value, pltpu.VMEM)


def slot_match(routing_ref, experts, rows):
    tok_count = routing_ref.shape[1]
    shape = (experts * rows, tok_count)
    slot = lax.broadcasted_iota(jnp.int32, shape, 0)
    expert, place = slot // rows, slot % rows
    named = (routing_ref[0:1, :] == expert) | (routing_ref[1:2, :] == expert)
    square = (tok_count, tok_count)
    earlier = lax.broadcasted_iota(jnp.int32, square, 0) < lax.broadcasted_iota(jnp.int32, square, 1)
    before = jnp.dot(
        named.astype(F32).astype(BF), earlier.astype(F32).astype(BF), preferred_element_type=F32
    )
    return expert, named & (before == place.astype(F32))


def pack_kernel(experts, rows, routing_ref, tokens_ref, out_ref, whole_ref):
    hi_count, _, feat = tokens_ref.shape
    _, held = slot_match(routing_ref, experts, rows)
    dispatch = held.astype(F32).astype(BF)
    for i in range(hi_count):
        whole_ref[:, i * feat : (i + 1) * feat] = tokens_ref[i]
    packed = jnp.dot(dispatch, whole_ref[...], preferred_element_type=F32).astype(BF)
    for i in range(out_ref.shape[0]):
        out_ref[i] = packed


def ffn_kernel(got_ref, gate_ref, up_ref, down_ref, out_ref):
    lo_count = got_ref.shape[0]
    hi_count, _, feat, hidden_n = gate_ref.shape
    wide = hi_count * feat
    gate = up = 0.0
    for i in range(lo_count):
        gate += jnp.dot(
            got_ref[i], gate_ref[:, i].reshape(wide, hidden_n), preferred_element_type=F32
        )
        up += jnp.dot(got_ref[i], up_ref[:, i].reshape(wide, hidden_n), preferred_element_type=F32)
    hidden = (gate / (1.0 + jnp.exp(-gate)) * up).astype(BF)
    step = 4 * lo_count
    for k in range(hi_count * lo_count // step):
        block = jnp.dot(
            hidden, down_ref[:, k * step * feat : (k + 1) * step * feat], preferred_element_type=F32
        ).astype(BF)
        for j in range(step):
            place = (k * step + j) // lo_count * feat
            out_ref[j % lo_count, :, place : place + feat] = block[:, j * feat : (j + 1) * feat]


def combine_kernel(experts, rows, feat, routing_ref, gates_ref, back_ref, out_ref):
    tok_count = routing_ref.shape[1]
    hi_count = back_ref.shape[1] // feat
    expert, held = slot_match(routing_ref, experts, rows)
    weight = jnp.where(routing_ref[0:1, :] == expert, gates_ref[0:1, :], gates_ref[1:2, :])
    weight = jnp.where(held, weight, 0.0).astype(BF)
    weight = jnp.concatenate([weight] * LO, axis=0)
    mixed = lax.dot_general(
        weight, back_ref[...], (((0,), (0,)), ((), ())), preferred_element_type=F32
    )
    full = tok_count * 3 // 4
    for i in range(hi_count):
        at = (i,)
        block = mixed[:, i * feat : (i + 1) * feat]
        out_ref[*at, :, :feat] = block[:full].astype(BF)
        tail = [block[full:, j * (feat // 3) : (j + 1) * (feat // 3)] for j in range(3)]
        out_ref[*at, :, feat:] = jnp.concatenate(tail, axis=0).astype(BF)


def body(tokens, routing, route_gates, expert_gate, expert_up, expert_down):
    ep_count = lax.axis_size("ep")
    hi_count = lax.axis_size("hi")
    tok_count, feat = tokens.shape
    capacity = 2 * tok_count // ep_count + tok_count // 16
    rows = -(-capacity // 16) * 16
    slots = ep_count * rows
    wide = hi_count * feat
    hidden_n = expert_gate.shape[2]
    in_vmem = pl.BlockSpec(memory_space=pltpu.VMEM)

    gathered = lax.all_gather(tokens, "hi", axis=0)
    sent = pl.pallas_call(
        functools.partial(pack_kernel, ep_count, rows),
        out_shape=pltpu.VMEM((LO, slots, wide), BF),
        in_specs=[in_vmem, in_vmem],
        out_specs=in_vmem,
        scratch_shapes=[pltpu.VMEM((tok_count, wide), BF)],
        compiler_params=pltpu.CompilerParams(vmem_limit_bytes=16 << 20),
        name="pack",
    )(routing.T, held_close(gathered))
    got = lax.all_to_all(
        sent.reshape(LO * ep_count, rows, wide), ("lo", "ep"), 0, 0, tiled=True
    ).reshape(LO, slots, wide)

    part = pl.pallas_call(
        ffn_kernel,
        out_shape=pltpu.VMEM((LO, slots, wide), BF),
        in_specs=[in_vmem] * 4,
        out_specs=in_vmem,
        compiler_params=pltpu.CompilerParams(vmem_limit_bytes=16 << 20),
        name="ffn",
    )(
        held_close(got),
        held_close(expert_gate.reshape(hi_count, LO, feat, hidden_n)),
        held_close(expert_up.reshape(hi_count, LO, feat, hidden_n)),
        held_close(expert_down.reshape(hidden_n, LO * wide)),
    )
    back = lax.all_to_all(
        part.reshape(LO * ep_count, rows, wide), ("lo", "ep"), 0, 0, tiled=True
    ).reshape(LO * slots, wide)
    mixed = pl.pallas_call(
        functools.partial(combine_kernel, ep_count, rows, feat),
        out_shape=pltpu.VMEM((*(hi_count,), tok_count * 3 // 4, feat * 4 // 3), BF),
        in_specs=[in_vmem, in_vmem, in_vmem],
        out_specs=in_vmem,
        compiler_params=pltpu.CompilerParams(vmem_limit_bytes=16 << 20),
        name="combine",
    )(routing.T, route_gates.T, held_close(back))
    shares = lax.all_to_all(mixed, "hi", 0, 0, tiled=True)
    return pl.pallas_call(
        finish_kernel,
        out_shape=jax.ShapeDtypeStruct((tok_count, feat), BF),
        in_specs=[in_vmem],
        out_specs=in_vmem,
        compiler_params=pltpu.CompilerParams(vmem_limit_bytes=16 << 20),
        name="finish",
    )(held_close(shares))


def finish_kernel(shares_ref, out_ref):
    tok_count, feat = out_ref.shape
    full, cut = tok_count * 3 // 4, feat // 3
    total = jnp.sum(shares_ref[...].astype(F32), axis=0)
    out_ref[:full] = total[:, :feat].astype(BF)
    step = full // 3
    tail = [total[j * step : (j + 1) * step, feat:] for j in range(3)]
    out_ref[full:] = jnp.concatenate(tail, axis=1).astype(BF)


def solution(mesh):
    finer = Mesh(
        mesh.devices.reshape(
            mesh.shape["rep"], mesh.shape["tp"] // LO, LO, mesh.shape["ep"]
        ),
        ("rep", "hi", "lo", "ep"),
    )
    placed = (
        P(REP_EP, TP),
        P(REP_EP, None),
        P(REP_EP, None),
        P("ep", None, TP),
        P("ep", None, TP),
        P("ep", TP, None),
    )
    return jax.shard_map(
        body, mesh=finer, in_specs=placed, out_specs=P(REP_EP, TP), check_vma=False
    )
```

```python
import functools

import jax
import jax.numpy as jnp
from jax import lax
from jax.experimental import pallas as pl
from jax.experimental.pallas import tpu as pltpu
from jax.sharding import Mesh
from jax.sharding import PartitionSpec as P

REP_EP = ("rep", "ep")
HI = ("h3", "h2", "h1", "h0")
TP = (*HI, "lo")
BF = jnp.bfloat16
F32 = jnp.float32
LO = 2


def held_close(value):
    return pltpu.with_memory_space_constraint(value, pltpu.VMEM)


ORDER = (1, 0, 3, 2)


def mirrored(index):
    bits = f"{index:0{len(HI)}b}"
    return int("".join(bits[i] for i in ORDER), 2)


def slot_match(routing_ref, experts, rows):
    tok_count = routing_ref.shape[1]
    shape = (experts * rows, tok_count)
    slot = lax.broadcasted_iota(jnp.int32, shape, 0)
    expert, place = slot // rows, slot % rows
    named = (routing_ref[0:1, :] == expert) | (routing_ref[1:2, :] == expert)
    square = (tok_count, tok_count)
    earlier = lax.broadcasted_iota(jnp.int32, square, 0) < lax.broadcasted_iota(jnp.int32, square, 1)
    before = jnp.dot(
        named.astype(F32).astype(BF), earlier.astype(F32).astype(BF), preferred_element_type=F32
    )
    return expert, named & (before == place.astype(F32))


def pack_kernel(experts, rows, routing_ref, tokens_ref, out_ref, whole_ref):
    hi_count, _, feat = tokens_ref.shape
    _, held = slot_match(routing_ref, experts, rows)
    dispatch = held.astype(F32).astype(BF)
    for i in range(hi_count):
        whole_ref[:, i * feat : (i + 1) * feat] = tokens_ref[i]
    packed = jnp.dot(dispatch, whole_ref[...], preferred_element_type=F32).astype(BF)
    for i in range(out_ref.shape[0]):
        out_ref[i] = packed


def ffn_kernel(got_ref, gate_ref, up_ref, down_ref, out_ref):
    lo_count = got_ref.shape[0]
    hi_count, _, feat, hidden_n = gate_ref.shape
    wide = hi_count * feat
    gate = up = 0.0
    for i in range(lo_count):
        gate += jnp.dot(
            got_ref[i], gate_ref[:, i].reshape(wide, hidden_n), preferred_element_type=F32
        )
        up += jnp.dot(got_ref[i], up_ref[:, i].reshape(wide, hidden_n), preferred_element_type=F32)
    hidden = (gate / (1.0 + jnp.exp(-gate)) * up).astype(BF)
    step = 4 * lo_count
    for k in range(hi_count * lo_count // step):
        block = jnp.dot(
            hidden, down_ref[:, k * step * feat : (k + 1) * step * feat], preferred_element_type=F32
        ).astype(BF)
        for j in range(step):
            place = (k * step + j) // lo_count * feat
            out_ref[j % lo_count, :, place : place + feat] = block[:, j * feat : (j + 1) * feat]


def combine_kernel(experts, rows, feat, routing_ref, gates_ref, back_ref, out_ref):
    tok_count = routing_ref.shape[1]
    hi_count = back_ref.shape[1] // feat
    expert, held = slot_match(routing_ref, experts, rows)
    weight = jnp.where(routing_ref[0:1, :] == expert, gates_ref[0:1, :], gates_ref[1:2, :])
    weight = jnp.where(held, weight, 0.0).astype(BF)
    weight = jnp.concatenate([weight] * LO, axis=0)
    mixed = lax.dot_general(
        weight, back_ref[...], (((0,), (0,)), ((), ())), preferred_element_type=F32
    )
    full = tok_count * 3 // 4
    for i in range(hi_count):
        at = mirrored(i)
        block = mixed[:, i * feat : (i + 1) * feat]
        out_ref[at, :, :feat] = block[:full].astype(BF)
        tail = [block[full:, j * (feat // 3) : (j + 1) * (feat // 3)] for j in range(3)]
        out_ref[at, :, feat:] = jnp.concatenate(tail, axis=0).astype(BF)


def body(tokens, routing, route_gates, expert_gate, expert_up, expert_down):
    ep_count = lax.axis_size("ep")
    hi_count = lax.axis_size(HI)
    tok_count, feat = tokens.shape
    capacity = 2 * tok_count // ep_count + tok_count // 16
    rows = -(-capacity // 16) * 16
    slots = ep_count * rows
    wide = hi_count * feat
    hidden_n = expert_gate.shape[2]
    in_vmem = pl.BlockSpec(memory_space=pltpu.VMEM)

    gathered = lax.all_gather(tokens, HI, axis=0)
    sent = pl.pallas_call(
        functools.partial(pack_kernel, ep_count, rows),
        out_shape=pltpu.VMEM((LO, slots, wide), BF),
        in_specs=[in_vmem, in_vmem],
        out_specs=in_vmem,
        scratch_shapes=[pltpu.VMEM((tok_count, wide), BF)],
        compiler_params=pltpu.CompilerParams(vmem_limit_bytes=16 << 20),
        name="pack",
    )(routing.T, held_close(gathered))
    got = lax.all_to_all(
        sent.reshape(LO * ep_count, rows, wide), ("lo", "ep"), 0, 0, tiled=True
    ).reshape(LO, slots, wide)

    part = pl.pallas_call(
        ffn_kernel,
        out_shape=pltpu.VMEM((LO, slots, wide), BF),
        in_specs=[in_vmem] * 4,
        out_specs=in_vmem,
        compiler_params=pltpu.CompilerParams(vmem_limit_bytes=16 << 20),
        name="ffn",
    )(
        held_close(got),
        held_close(expert_gate.reshape(hi_count, LO, feat, hidden_n)),
        held_close(expert_up.reshape(hi_count, LO, feat, hidden_n)),
        held_close(expert_down.reshape(hidden_n, LO * wide)),
    )
    back = lax.all_to_all(
        part.reshape(LO * ep_count, rows, wide), ("lo", "ep"), 0, 0, tiled=True
    ).reshape(LO * slots, wide)
    mixed = pl.pallas_call(
        functools.partial(combine_kernel, ep_count, rows, feat),
        out_shape=pltpu.VMEM((hi_count, tok_count * 3 // 4, feat * 4 // 3), BF),
        in_specs=[in_vmem, in_vmem, in_vmem],
        out_specs=in_vmem,
        compiler_params=pltpu.CompilerParams(vmem_limit_bytes=16 << 20),
        name="combine",
    )(routing.T, route_gates.T, held_close(back))
    shares = lax.all_to_all(mixed, tuple(HI[i] for i in ORDER), 0, 0, tiled=True)
    return pl.pallas_call(
        finish_kernel,
        out_shape=jax.ShapeDtypeStruct((tok_count, feat), BF),
        in_specs=[in_vmem],
        out_specs=in_vmem,
        compiler_params=pltpu.CompilerParams(vmem_limit_bytes=16 << 20),
        name="finish",
    )(held_close(shares))


def finish_kernel(shares_ref, out_ref):
    tok_count, feat = out_ref.shape
    full, cut = tok_count * 3 // 4, feat // 3
    total = jnp.sum(shares_ref[...].astype(F32), axis=0)
    out_ref[:full] = total[:, :feat].astype(BF)
    step = full // 3
    tail = [total[j * step : (j + 1) * step, feat:] for j in range(3)]
    out_ref[full:] = jnp.concatenate(tail, axis=1).astype(BF)


def solution(mesh):
    finer = Mesh(
        mesh.devices.reshape(
            mesh.shape["rep"], *[2] * len(HI), LO, mesh.shape["ep"]
        ),
        ("rep", *TP, "ep"),
    )
    placed = (
        P(REP_EP, TP),
        P(REP_EP, None),
        P(REP_EP, None),
        P("ep", None, TP),
        P("ep", None, TP),
        P("ep", TP, None),
    )
    return jax.shard_map(
        body, mesh=finer, in_specs=placed, out_specs=P(REP_EP, TP), check_vma=False
    )
```

```python
import functools

import jax
import jax.numpy as jnp
from jax import lax
from jax.experimental import pallas as pl
from jax.experimental.pallas import tpu as pltpu
from jax.sharding import Mesh
from jax.sharding import PartitionSpec as P

REP_EP = ("rep", "ep")
HI = ("h3", "h2", "h1", "h0")
TP = (*HI, "lo")
BF = jnp.bfloat16
F32 = jnp.float32
LO = 2


def held_close(value):
    return pltpu.with_memory_space_constraint(value, pltpu.VMEM)


ORDER = (1, 0, 3, 2)


def mirrored(index):
    bits = f"{index:0{len(HI)}b}"
    return int("".join(bits[i] for i in ORDER), 2)


def slot_match(routing_ref, experts, rows):
    tok_count = routing_ref.shape[1]
    shape = (experts * rows, tok_count)
    slot = lax.broadcasted_iota(jnp.int32, shape, 0)
    expert, place = slot // rows, slot % rows
    named = (routing_ref[0:1, :] == expert) | (routing_ref[1:2, :] == expert)
    square = (tok_count, tok_count)
    earlier = lax.broadcasted_iota(jnp.int32, square, 0) < lax.broadcasted_iota(jnp.int32, square, 1)
    before = jnp.dot(
        named.astype(F32).astype(BF), earlier.astype(F32).astype(BF), preferred_element_type=F32
    )
    return expert, named & (before == place.astype(F32))


def folded(value, full):
    part, step = value.shape[1] // 4, full // 4
    tail = [value[full : full + step, i * part : (i + 1) * part] for i in range(4)]
    return jnp.concatenate([value[:full], jnp.concatenate(tail, axis=0)], axis=1).astype(BF)


def unfolded(value, rows):
    full, part = value.shape[0], value.shape[1] // 5
    step = full // 4
    value = value.astype(F32)
    tail = [value[i * step : (i + 1) * step, 4 * part :] for i in range(4)]
    spare = jnp.zeros((rows - full - step, 4 * part), F32)
    return jnp.concatenate(
        [value[:, : 4 * part], jnp.concatenate([jnp.concatenate(tail, axis=1), spare], axis=0)], axis=0
    ).astype(BF)


def pack_kernel(experts, rows, routing_ref, tokens_ref, out_ref, whole_ref):
    hi_count, _, feat = tokens_ref.shape
    _, held = slot_match(routing_ref, experts, rows)
    dispatch = held.astype(F32).astype(BF)
    for i in range(hi_count):
        whole_ref[:, i * feat : (i + 1) * feat] = tokens_ref[i]
    packed = jnp.dot(dispatch, whole_ref[...], preferred_element_type=F32)
    for e in range(experts):
        piece = folded(packed[e * rows : (e + 1) * rows], out_ref.shape[2])
        for i in range(out_ref.shape[0]):
            out_ref[i, e] = piece


def ffn_kernel(rows, got_ref, gate_ref, up_ref, down_ref, out_ref, got_rows, part_rows):
    lo_count, experts, full, _ = got_ref.shape
    for i in range(lo_count):
        for e in range(experts):
            got_rows[i, e * rows : (e + 1) * rows] = unfolded(got_ref[i, e], rows)
    hi_count, _, feat, hidden_n = gate_ref.shape
    wide = hi_count * feat
    gate = up = 0.0
    for i in range(lo_count):
        gate += jnp.dot(
            got_rows[i], gate_ref[:, i].reshape(wide, hidden_n), preferred_element_type=F32
        )
        up += jnp.dot(got_rows[i], up_ref[:, i].reshape(wide, hidden_n), preferred_element_type=F32)
    hidden = (gate / (1.0 + jnp.exp(-gate)) * up).astype(BF)
    step = 4 * lo_count
    for k in range(hi_count * lo_count // step):
        block = jnp.dot(
            hidden, down_ref[:, k * step * feat : (k + 1) * step * feat], preferred_element_type=F32
        )
        for j in range(step):
            place = (k * step + j) // lo_count * feat
            part_rows[j % lo_count, :, place : place + feat] = block[:, j * feat : (j + 1) * feat]
    for i in range(lo_count):
        for e in range(experts):
            out_ref[i, e] = folded(part_rows[i, e * rows : (e + 1) * rows], full)


def combine_kernel(experts, rows, feat, routing_ref, gates_ref, back_ref, out_ref, back_rows):
    tok_count = routing_ref.shape[1]
    hi_count = back_rows.shape[1] // feat
    for i in range(LO * experts):
        back_rows[i * rows : (i + 1) * rows] = unfolded(back_ref[i], rows)
    expert, held = slot_match(routing_ref, experts, rows)
    weight = jnp.where(routing_ref[0:1, :] == expert, gates_ref[0:1, :], gates_ref[1:2, :])
    weight = jnp.where(held, weight, 0.0).astype(BF)
    weight = jnp.concatenate([weight] * LO, axis=0)
    mixed = lax.dot_general(
        weight, back_rows[...], (((0,), (0,)), ((), ())), preferred_element_type=F32
    )
    full = tok_count * 3 // 4
    for i in range(hi_count):
        at = mirrored(i)
        block = mixed[:, i * feat : (i + 1) * feat]
        out_ref[at, :, :feat] = block[:full].astype(BF)
        tail = [block[full:, j * (feat // 3) : (j + 1) * (feat // 3)] for j in range(3)]
        out_ref[at, :, feat:] = jnp.concatenate(tail, axis=0).astype(BF)


def body(tokens, routing, route_gates, expert_gate, expert_up, expert_down):
    ep_count = lax.axis_size("ep")
    hi_count = lax.axis_size(HI)
    tok_count, feat = tokens.shape
    capacity = 2 * tok_count // ep_count + tok_count // 16
    rows = -(-capacity // 16) * 16
    slots = ep_count * rows
    wide = hi_count * feat
    full = capacity * 4 // 5
    piece = (full, wide * 5 // 4)
    hidden_n = expert_gate.shape[2]
    in_vmem = pl.BlockSpec(memory_space=pltpu.VMEM)

    gathered = lax.all_gather(tokens, HI, axis=0)
    sent = pl.pallas_call(
        functools.partial(pack_kernel, ep_count, rows),
        out_shape=pltpu.VMEM((LO, ep_count, *piece), BF),
        in_specs=[in_vmem, in_vmem],
        out_specs=in_vmem,
        scratch_shapes=[pltpu.VMEM((tok_count, wide), BF)],
        compiler_params=pltpu.CompilerParams(vmem_limit_bytes=16 << 20),
        name="pack",
    )(routing.T, held_close(gathered))
    got = lax.all_to_all(
        sent.reshape(LO * ep_count, *piece), ("lo", "ep"), 0, 0, tiled=True
    ).reshape(LO, ep_count, *piece)

    part = pl.pallas_call(
        functools.partial(ffn_kernel, rows),
        out_shape=pltpu.VMEM((LO, ep_count, *piece), BF),
        in_specs=[in_vmem] * 4,
        out_specs=in_vmem,
        scratch_shapes=[pltpu.VMEM((LO, slots, wide), BF), pltpu.VMEM((LO, slots, wide), F32)],
        compiler_params=pltpu.CompilerParams(vmem_limit_bytes=16 << 20),
        name="ffn",
    )(
        held_close(got),
        held_close(expert_gate.reshape(hi_count, LO, feat, hidden_n)),
        held_close(expert_up.reshape(hi_count, LO, feat, hidden_n)),
        held_close(expert_down.reshape(hidden_n, LO * wide)),
    )
    back = lax.all_to_all(
        part.reshape(LO * ep_count, *piece), ("lo", "ep"), 0, 0, tiled=True
    )
    mixed = pl.pallas_call(
        functools.partial(combine_kernel, ep_count, rows, feat),
        out_shape=pltpu.VMEM((hi_count, tok_count * 3 // 4, feat * 4 // 3), BF),
        in_specs=[in_vmem, in_vmem, in_vmem],
        out_specs=in_vmem,
        scratch_shapes=[pltpu.VMEM((LO * slots, wide), BF)],
        compiler_params=pltpu.CompilerParams(vmem_limit_bytes=16 << 20),
        name="combine",
    )(routing.T, route_gates.T, held_close(back))
    shares = lax.all_to_all(mixed, tuple(HI[i] for i in ORDER), 0, 0, tiled=True)
    return pl.pallas_call(
        finish_kernel,
        out_shape=jax.ShapeDtypeStruct((tok_count, feat), BF),
        in_specs=[in_vmem],
        out_specs=in_vmem,
        compiler_params=pltpu.CompilerParams(vmem_limit_bytes=16 << 20),
        name="finish",
    )(held_close(shares))


def finish_kernel(shares_ref, out_ref):
    tok_count, feat = out_ref.shape
    full, cut = tok_count * 3 // 4, feat // 3
    total = jnp.sum(shares_ref[...].astype(F32), axis=0)
    out_ref[:full] = total[:, :feat].astype(BF)
    step = full // 3
    tail = [total[j * step : (j + 1) * step, feat:] for j in range(3)]
    out_ref[full:] = jnp.concatenate(tail, axis=1).astype(BF)


def solution(mesh):
    finer = Mesh(
        mesh.devices.reshape(
            mesh.shape["rep"], *[2] * len(HI), LO, mesh.shape["ep"]
        ),
        ("rep", *TP, "ep"),
    )
    placed = (
        P(REP_EP, TP),
        P(REP_EP, None),
        P(REP_EP, None),
        P("ep", None, TP),
        P("ep", None, TP),
        P("ep", TP, None),
    )
    return jax.shard_map(
        body, mesh=finer, in_specs=placed, out_specs=P(REP_EP, TP), check_vma=False
    )
```

```python
import functools

import jax
import jax.numpy as jnp
from jax import lax
from jax.experimental import pallas as pl
from jax.experimental.pallas import tpu as pltpu
from jax.sharding import Mesh
from jax.sharding import PartitionSpec as P

REP_EP = ("rep", "ep")
HI = ("h3", "h2", "h1", "h0")
TP = (*HI, "lo")
BF = jnp.bfloat16
F32 = jnp.float32
LO = 2


def held_close(value):
    return pltpu.with_memory_space_constraint(value, pltpu.VMEM)


ORDER = [0, 3, 1, 2, 8, 11, 9, 10, 4, 7, 5, 6, 12, 15, 13, 14]


def mirrored(index):
    return ORDER.index(index)


def slot_match(routing_ref, experts, rows):
    tok_count = routing_ref.shape[1]
    shape = (experts * rows, tok_count)
    slot = lax.broadcasted_iota(jnp.int32, shape, 0)
    expert, place = slot // rows, slot % rows
    named = (routing_ref[0:1, :] == expert) | (routing_ref[1:2, :] == expert)
    square = (tok_count, tok_count)
    earlier = lax.broadcasted_iota(jnp.int32, square, 0) < lax.broadcasted_iota(jnp.int32, square, 1)
    before = jnp.dot(
        named.astype(F32).astype(BF), earlier.astype(F32).astype(BF), preferred_element_type=F32
    )
    return expert, named & (before == place.astype(F32))


def folded(value, full):
    part, step = value.shape[1] // 4, full // 4
    tail = [value[full : full + step, i * part : (i + 1) * part] for i in range(4)]
    return jnp.concatenate([value[:full], jnp.concatenate(tail, axis=0)], axis=1).astype(BF)


def unfolded(value, rows):
    full, part = value.shape[0], value.shape[1] // 5
    step = full // 4
    value = value.astype(F32)
    tail = [value[i * step : (i + 1) * step, 4 * part :] for i in range(4)]
    spare = jnp.zeros((rows - full - step, 4 * part), F32)
    return jnp.concatenate(
        [value[:, : 4 * part], jnp.concatenate([jnp.concatenate(tail, axis=1), spare], axis=0)], axis=0
    ).astype(BF)


def stage_kernel(experts, rows, routing_ref, tokens_ref, held_ref, out_ref, sem):
    copy = pltpu.make_async_copy(tokens_ref, out_ref, sem)
    copy.start()
    _, held = slot_match(routing_ref, experts, rows)
    held_ref[...] = held.astype(F32).astype(BF)
    copy.wait()


def pack_kernel(experts, rows, dispatch_ref, tokens_ref, out_ref, whole_ref):
    hi_count, _, feat = tokens_ref.shape
    for i in range(hi_count):
        whole_ref[:, i * feat : (i + 1) * feat] = tokens_ref[i]
    packed = jnp.dot(dispatch_ref[...], whole_ref[...], preferred_element_type=F32)
    for e in range(experts):
        piece = folded(packed[e * rows : (e + 1) * rows], out_ref.shape[2])
        for i in range(out_ref.shape[0]):
            out_ref[i, e] = piece


def ffn_kernel(rows, got_ref, gate_ref, up_ref, down_ref, out_ref, got_rows, part_rows):
    lo_count, experts, full, _ = got_ref.shape
    for i in range(lo_count):
        for e in range(experts):
            got_rows[i, e * rows : (e + 1) * rows] = unfolded(got_ref[i, e], rows)
    hi_count, _, feat, hidden_n = gate_ref.shape
    wide = hi_count * feat
    gate = up = 0.0
    for i in range(lo_count):
        gate += jnp.dot(
            got_rows[i], gate_ref[:, i].reshape(wide, hidden_n), preferred_element_type=F32
        )
        up += jnp.dot(got_rows[i], up_ref[:, i].reshape(wide, hidden_n), preferred_element_type=F32)
    hidden = (gate / (1.0 + jnp.exp(-gate)) * up).astype(BF)
    step = 4 * lo_count
    for k in range(hi_count * lo_count // step):
        block = jnp.dot(
            hidden, down_ref[:, k * step * feat : (k + 1) * step * feat], preferred_element_type=F32
        )
        for j in range(step):
            place = (k * step + j) // lo_count * feat
            part_rows[j % lo_count, :, place : place + feat] = block[:, j * feat : (j + 1) * feat]
    for i in range(lo_count):
        for e in range(experts):
            out_ref[i, e] = folded(part_rows[i, e * rows : (e + 1) * rows], full)


def combine_kernel(experts, rows, feat, routing_ref, gates_ref, back_ref, out_ref, back_rows):
    tok_count = routing_ref.shape[1]
    hi_count = back_rows.shape[1] // feat
    for i in range(LO * experts):
        back_rows[i * rows : (i + 1) * rows] = unfolded(back_ref[i], rows)
    expert, held = slot_match(routing_ref, experts, rows)
    weight = jnp.where(routing_ref[0:1, :] == expert, gates_ref[0:1, :], gates_ref[1:2, :])
    weight = jnp.where(held, weight, 0.0).astype(BF)
    weight = jnp.concatenate([weight] * LO, axis=0)
    mixed = lax.dot_general(
        weight, back_rows[...], (((0,), (0,)), ((), ())), preferred_element_type=F32
    )
    full = tok_count * 3 // 4
    for i in range(hi_count):
        at = mirrored(i)
        block = mixed[:, i * feat : (i + 1) * feat]
        out_ref[at, :, :feat] = block[:full].astype(BF)
        tail = [block[full:, j * (feat // 3) : (j + 1) * (feat // 3)] for j in range(3)]
        out_ref[at, :, feat:] = jnp.concatenate(tail, axis=0).astype(BF)


def body(tokens, routing, route_gates, expert_gate, expert_up, expert_down):
    ep_count = lax.axis_size("ep")
    hi_count = lax.axis_size(HI)
    tok_count, feat = tokens.shape
    capacity = 2 * tok_count // ep_count + tok_count // 16
    rows = -(-capacity // 16) * 16
    slots = ep_count * rows
    wide = hi_count * feat
    full = capacity * 4 // 5
    piece = (full, wide * 5 // 4)
    hidden_n = expert_gate.shape[2]
    in_vmem = pl.BlockSpec(memory_space=pltpu.VMEM)

    dispatch, staged = pl.pallas_call(
        functools.partial(stage_kernel, ep_count, rows),
        out_shape=(pltpu.VMEM((slots, tok_count), BF), pltpu.VMEM((tok_count, feat), BF)),
        in_specs=[in_vmem, pl.BlockSpec(memory_space=pl.ANY)],
        out_specs=(in_vmem, in_vmem),
        scratch_shapes=[pltpu.SemaphoreType.DMA],
        compiler_params=pltpu.CompilerParams(vmem_limit_bytes=16 << 20),
        name="stage",
    )(routing.T, pltpu.with_memory_space_constraint(tokens, pltpu.HBM))
    gathered = lax.all_gather(staged, HI, axis=0)
    sent = pl.pallas_call(
        functools.partial(pack_kernel, ep_count, rows),
        out_shape=pltpu.VMEM((LO, ep_count, *piece), BF),
        in_specs=[in_vmem, in_vmem],
        out_specs=in_vmem,
        scratch_shapes=[pltpu.VMEM((tok_count, wide), BF)],
        compiler_params=pltpu.CompilerParams(vmem_limit_bytes=16 << 20),
        name="pack",
    )(held_close(dispatch), held_close(gathered))
    got = lax.all_to_all(
        sent.reshape(LO * ep_count, *piece), ("lo", "ep"), 0, 0, tiled=True
    ).reshape(LO, ep_count, *piece)

    part = pl.pallas_call(
        functools.partial(ffn_kernel, rows),
        out_shape=pltpu.VMEM((LO, ep_count, *piece), BF),
        in_specs=[in_vmem] * 4,
        out_specs=in_vmem,
        scratch_shapes=[pltpu.VMEM((LO, slots, wide), BF), pltpu.VMEM((LO, slots, wide), F32)],
        compiler_params=pltpu.CompilerParams(vmem_limit_bytes=16 << 20),
        name="ffn",
    )(
        held_close(got),
        held_close(expert_gate.reshape(hi_count, LO, feat, hidden_n)),
        held_close(expert_up.reshape(hi_count, LO, feat, hidden_n)),
        held_close(expert_down.reshape(hidden_n, LO * wide)),
    )
    back = lax.all_to_all(
        part.reshape(LO * ep_count, *piece), ("lo", "ep"), 0, 0, tiled=True
    )
    mixed = pl.pallas_call(
        functools.partial(combine_kernel, ep_count, rows, feat),
        out_shape=pltpu.VMEM((hi_count, tok_count * 3 // 4, feat * 4 // 3), BF),
        in_specs=[in_vmem, in_vmem, in_vmem],
        out_specs=in_vmem,
        scratch_shapes=[pltpu.VMEM((LO * slots, wide), BF)],
        compiler_params=pltpu.CompilerParams(vmem_limit_bytes=16 << 20),
        name="combine",
    )(routing.T, route_gates.T, held_close(back))
    shares = lax.all_to_all(mixed, TP, 0, 0, tiled=True, axis_index_groups=[[LO * i + j for i in ORDER] for j in range(LO)])
    return pl.pallas_call(
        finish_kernel,
        out_shape=jax.ShapeDtypeStruct((tok_count, feat), BF),
        in_specs=[in_vmem],
        out_specs=in_vmem,
        compiler_params=pltpu.CompilerParams(vmem_limit_bytes=16 << 20),
        name="finish",
    )(held_close(shares))


def finish_kernel(shares_ref, out_ref):
    tok_count, feat = out_ref.shape
    full, cut = tok_count * 3 // 4, feat // 3
    total = jnp.sum(shares_ref[...].astype(F32), axis=0)
    out_ref[:full] = total[:, :feat].astype(BF)
    step = full // 3
    tail = [total[j * step : (j + 1) * step, feat:] for j in range(3)]
    out_ref[full:] = jnp.concatenate(tail, axis=1).astype(BF)


def solution(mesh):
    finer = Mesh(
        mesh.devices.reshape(
            mesh.shape["rep"], *[2] * len(HI), LO, mesh.shape["ep"]
        ),
        ("rep", *TP, "ep"),
    )
    placed = (
        P(REP_EP, TP),
        P(REP_EP, None),
        P(REP_EP, None),
        P("ep", None, TP),
        P("ep", None, TP),
        P("ep", TP, None),
    )
    return jax.shard_map(
        body, mesh=finer, in_specs=placed, out_specs=P(REP_EP, TP), check_vma=False
    )
```
